8 devices in a mesh: dp: 1 (over z), cp: 8 (over y, x, core).
Axes of the slice: x: 2, y: 2, z: 1, core: 2. Of those that a mesh axis runs over, the one named last changes fastest.
Arguments:
- hidden: bfloat16 [8, 1024, 3840], P('dp', 'cp')
- grad_out: bfloat16 [8, 1024, 3840], P('dp', 'cp')
- norm_gain: float32 [2, 3840], replicated
- w_qkv: bfloat16 [2, 3840, 8192], replicated
- b_qkv: float32 [2, 8192], replicated
- w_out: bfloat16 [2, 4096, 3840], replicated
- b_out: float32 [2, 3840], replicated
- attn_sinks: float32 [2, 16], replicated
Outputs:
- output 1: bfloat16 [8, 1024, 3840], P('dp', 'cp')
- output 2: bfloat16 [8, 1024, 3840], P('dp', 'cp')
- output 3: float32 [8, 2, 3840], P(('dp', 'cp'))
- output 4: float32 [8, 2, 8192], P(('dp', 'cp'))
- output 5: float32 [8, 2, 3840], P(('dp', 'cp'))
- output 6: float32 [8, 2, 16], P(('dp', 'cp'))
All inputs are finite; a program needn't handle non-finite values.
Results may differ from the reference program's by a relative error of at most 0.02.
Values are sent between devices in bfloat16 or wider.
A program may use at most 1 GiB of HBM per device.

```python
import jax
import jax.numpy as jnp
import math
from jax import lax

BATCH = 8
SEQ = 1024
CHUNKS = 8
D = 3840
HEADS = 16
KV_HEADS = 8
HEAD = 256
WINDOW = 128
SEQ_DEV = SEQ // CHUNKS
GROUP = HEADS // KV_HEADS
Q_WIDTH = HEADS * HEAD
K_WIDTH = KV_HEADS * HEAD
QKV = Q_WIDTH + 2 * K_WIDTH
SCALE = HEAD ** -0.5
EPSILON = 1e-5
ROPE_THETA = 150000.0
YARN_FACTOR = 32.0
YARN_CONTEXT = 4096.0
YARN_ALPHA = 1.0
YARN_BETA = 32.0


def rope_tables(positions):
    half_dim = HEAD // 2
    freq_steps = jnp.arange(half_dim, dtype=jnp.float32)
    freq_base = ROPE_THETA ** (freq_steps * 2.0 / HEAD)
    concentration = 0.1 * math.log(YARN_FACTOR) + 1.0
    low_edge = half_dim * math.log(YARN_CONTEXT / (YARN_BETA * 2.0 * math.pi)) / math.log(ROPE_THETA)
    high_edge = half_dim * math.log(YARN_CONTEXT / (YARN_ALPHA * 2.0 * math.pi)) / math.log(ROPE_THETA)
    ramp_pos = jnp.clip((freq_steps - low_edge) / (high_edge - low_edge), 0.0, 1.0)
    inv_freq = (1.0 - ramp_pos) / freq_base + ramp_pos / (YARN_FACTOR * freq_base)
    angles = positions.astype(jnp.float32)[:, None] * inv_freq[None, :]
    return jnp.cos(angles) * concentration, jnp.sin(angles) * concentration


def rotate_half(tensor, cos_tab, sin_tab):
    half_dim = tensor.shape[-1] // 2
    first_half = tensor[..., :half_dim]
    second_half = tensor[..., half_dim:]
    return jnp.concatenate([first_half * cos_tab - second_half * sin_tab, second_half * cos_tab + first_half * sin_tab], axis=-1)


def attention_layer(hidden, gain_c, w_in, bias_c, w_proj, bout_c, sink_c, cos_tab, sin_tab, window_on):
    hid_f = hidden.astype(jnp.float32)
    inv_rms = lax.rsqrt(jnp.mean(hid_f * hid_f, axis=-1, keepdims=True) + EPSILON)
    normed = ((hid_f * inv_rms).reshape(BATCH, CHUNKS, SEQ_DEV, D) * gain_c[None, :, None, :]).reshape(BATCH, SEQ, D).astype(jnp.bfloat16)
    projected = jnp.dot(normed, w_in, preferred_element_type=jnp.float32)
    projected = (projected.reshape(BATCH, CHUNKS, SEQ_DEV, QKV) + bias_c[None, :, None, :]).reshape(BATCH, SEQ, QKV)
    query_rows = rotate_half(projected[..., :Q_WIDTH].reshape(BATCH, SEQ, KV_HEADS, GROUP, HEAD), cos_tab[:, None, None, :], sin_tab[:, None, None, :]).astype(jnp.bfloat16)
    key_rows = rotate_half(projected[..., Q_WIDTH:Q_WIDTH + K_WIDTH].reshape(BATCH, SEQ, KV_HEADS, HEAD), cos_tab[:, None, :], sin_tab[:, None, :]).astype(jnp.bfloat16)
    value_rows = projected[..., Q_WIDTH + K_WIDTH:].reshape(BATCH, SEQ, KV_HEADS, HEAD).astype(jnp.bfloat16)
    positions = jnp.arange(SEQ)
    query_blocks = jnp.moveaxis(query_rows.reshape(BATCH, CHUNKS, SEQ_DEV, KV_HEADS, GROUP, HEAD), 1, 0)
    row_blocks = positions.reshape(CHUNKS, SEQ_DEV)
    sink_blocks = sink_c.reshape(CHUNKS, KV_HEADS, GROUP)
    keys_f = key_rows.astype(jnp.float32)
    values_f = value_rows.astype(jnp.float32)

    def one_block(block_args):
        query_blk, row_pos, sink_row = block_args
        scores = SCALE * jnp.einsum('bqkgd,bskd->bkgqs', query_blk.astype(jnp.float32), keys_f)
        allowed = positions[None, :] <= row_pos[:, None]
        if window_on:
            allowed = allowed & (positions[None, :] >= row_pos[:, None] - WINDOW)
        scores = jnp.where(allowed, scores, -jnp.inf)
        sink_grid = sink_row[None, :, :, None]
        row_peak = lax.stop_gradient(jnp.maximum(jnp.max(scores, axis=-1), sink_grid))
        exp_scores = jnp.exp(scores - row_peak[..., None])
        denominator = jnp.sum(exp_scores, axis=-1) + jnp.exp(sink_grid - row_peak)
        prob_bf = (exp_scores / denominator[..., None]).astype(jnp.bfloat16)
        return jnp.einsum('bkgqs,bskd->bqkgd', prob_bf.astype(jnp.float32), values_f).astype(jnp.bfloat16)

    attn_out = lax.map(jax.checkpoint(one_block), (query_blocks, row_blocks, sink_blocks))
    attn_out = jnp.moveaxis(attn_out, 0, 1).reshape(BATCH, SEQ, Q_WIDTH)
    out_proj = jnp.dot(attn_out, w_proj, preferred_element_type=jnp.float32)
    out_proj = (out_proj.reshape(BATCH, CHUNKS, SEQ_DEV, D) + bout_c[None, :, None, :]).reshape(BATCH, SEQ, D)
    return (hid_f + out_proj).astype(jnp.bfloat16)


def setup_inputs(seed: int = 0, part: int = 0) -> dict:
    part_key = jax.random.fold_in(jax.random.key(seed), part)
    key_hidden, key_grad = jax.random.split(part_key)
    shared = jax.random.split(jax.random.key(seed + 1), 6)
    hidden = jax.random.normal(key_hidden, (BATCH, SEQ, D), jnp.float32).astype(jnp.bfloat16)
    grad_out = jax.random.normal(key_grad, (BATCH, SEQ, D), jnp.float32).astype(jnp.bfloat16)
    norm_gain = 1.0 + 0.3 * jax.random.normal(shared[0], (2, D), jnp.float32)
    w_qkv = (jax.random.normal(shared[1], (2, D, QKV), jnp.float32) * D ** -0.5).astype(jnp.bfloat16)
    b_qkv = 0.3 * jax.random.normal(shared[2], (2, QKV), jnp.float32)
    w_out = (jax.random.normal(shared[3], (2, Q_WIDTH, D), jnp.float32) * Q_WIDTH ** -0.5).astype(jnp.bfloat16)
    b_out = 0.3 * jax.random.normal(shared[4], (2, D), jnp.float32)
    sink_base = jnp.array([math.log(WINDOW + 1.0), math.log(SEQ / 2.0)], jnp.float32)[:, None] + 1.0
    attn_sinks = sink_base + jax.random.normal(shared[5], (2, HEADS), jnp.float32)
    return {'hidden': hidden, 'grad_out': grad_out, 'norm_gain': norm_gain, 'w_qkv': w_qkv, 'b_qkv': b_qkv, 'w_out': w_out, 'b_out': b_out, 'attn_sinks': attn_sinks}


def reference(hidden, grad_out, norm_gain, w_qkv, b_qkv, w_out, b_out, attn_sinks):
    cos_tab, sin_tab = rope_tables(jnp.arange(SEQ))

    def forward(hid_in, gain_t, bias_t, bout_t, sink_t):
        middle = attention_layer(hid_in, gain_t[0], w_qkv[0], bias_t[0], w_out[0], bout_t[0], sink_t[0], cos_tab, sin_tab, True)
        return attention_layer(middle, gain_t[1], w_qkv[1], bias_t[1], w_out[1], bout_t[1], sink_t[1], cos_tab, sin_tab, False)

    def tile_rows(row_table):
        return jnp.broadcast_to(row_table[:, None, :], (2, CHUNKS, row_table.shape[-1]))

    output, pullback = jax.vjp(forward, hidden, tile_rows(norm_gain), tile_rows(b_qkv), tile_rows(b_out), tile_rows(attn_sinks))
    d_hidden, d_gain, d_bias, d_bout, d_sink = pullback(grad_out)
    return output, d_hidden, jnp.swapaxes(d_gain, 0, 1), jnp.swapaxes(d_bias, 0, 1), jnp.swapaxes(d_bout, 0, 1), jnp.swapaxes(d_sink, 0, 1)
```

```python
import functools
import jax
import jax.numpy as jnp
import math
from jax import lax
from jax.experimental import pallas as pl
from jax.experimental.pallas import tpu as pltpu
from jax.sharding import PartitionSpec as P

EPSILON = 1e-5
ROPE_THETA = 150000.0
YARN_FACTOR = 32.0
YARN_CONTEXT = 4096.0
YARN_ALPHA = 1.0
YARN_BETA = 32.0
LOG2E = 1.4426950408889634
VMEM_LIMIT = 66_000_000
BF = jnp.bfloat16
F32 = jnp.float32


def rope_tables(positions, head_dim):
    half_dim = head_dim // 2
    freq_steps = jnp.arange(half_dim, dtype=jnp.float32)
    freq_base = ROPE_THETA ** (freq_steps * 2.0 / head_dim)
    concentration = 0.1 * math.log(YARN_FACTOR) + 1.0
    low_edge = half_dim * math.log(YARN_CONTEXT / (YARN_BETA * 2.0 * math.pi)) / math.log(ROPE_THETA)
    high_edge = half_dim * math.log(YARN_CONTEXT / (YARN_ALPHA * 2.0 * math.pi)) / math.log(ROPE_THETA)
    ramp_pos = jnp.clip((freq_steps - low_edge) / (high_edge - low_edge), 0.0, 1.0)
    inv_freq = (1.0 - ramp_pos) / freq_base + ramp_pos / (YARN_FACTOR * freq_base)
    angles = positions.astype(jnp.float32)[:, None] * inv_freq[None, :]
    return jnp.cos(angles) * concentration, jnp.sin(angles) * concentration


def dot_nn(a, b):
    return lax.dot_general(a, b, (((1,), (0,)), ((), ())), preferred_element_type=F32)


def dot_nt(a, b):
    return lax.dot_general(a, b, (((1,), (1,)), ((), ())), preferred_element_type=F32)


def dot_tn(a, b):
    return lax.dot_general(a, b, (((0,), (0,)), ((), ())), preferred_element_type=F32)


def rotate(block, cos, sin):
    half = block.shape[1] // 2
    lo, hi = block[:, :half], block[:, half:]
    return jnp.concatenate([lo * cos - hi * sin, hi * cos + lo * sin], axis=1)


def window_mask(keys, cols):
    key = lax.broadcasted_iota(jnp.int32, (keys, cols), 0) + (256 - keys)
    row = lax.rem(lax.broadcasted_iota(jnp.int32, (keys, cols), 1), 128)
    return (key >= row) & (key <= row + 128)


def causal_mask(size, cols):
    key = lax.broadcasted_iota(jnp.int32, (size, cols), 0)
    row = lax.rem(lax.broadcasted_iota(jnp.int32, (size, cols), 1), size)
    return key <= row


def spans(window_on, rows):
    if window_on:
        return [(r, 128, max(r - 128, 0), r + 128, min(256, r + 128)) for r in range(0, rows, 128)][::-1]
    return [(r, 256, 0, r + 256, 256) for r in range(0, rows, 256)][::-1]


def masked_logits(s, mask, count):
    if count == s.shape[0]:
        return jnp.where(mask, s, -jnp.inf)
    return jnp.concatenate([s[:-count], jnp.where(mask, s[-count:], -jnp.inf)], axis=0)


def forward_kernel(layer, window_on, scale, x_ref, gain_ref, wq_ref, wk_ref, wv_ref, bq_ref, bk_ref, bv_ref, cos_ref, sin_ref, sink_ref, q_ref, k_ref, v_ref, o_ref, lse_ref, n_ref):
    head = pl.program_id(0)
    rows = x_ref.shape[0]
    hd = k_ref.shape[1]

    @pl.when(head == 0)
    def _():
        def norm(i, c):
            part = pl.ds(pl.multiple_of(i * 64, 64), 64)
            f = x_ref[part, :].astype(F32)
            inv = lax.rsqrt(jnp.mean(f * f, axis=1, keepdims=True) + EPSILON)
            n_ref[part, :] = (f * inv * gain_ref[...]).astype(BF)
            return c

        lax.fori_loop(0, rows // 64, norm, 0)

    step = min(512, rows)
    for r in range(0, rows, step):
        part = slice(r, r + step)
        n = n_ref[part, :]
        cos, sin = cos_ref[part, :], sin_ref[part, :]
        tq = dot_nn(n, wq_ref[...]) + bq_ref[...]
        q_ref[part, :hd] = rotate(tq[:, :hd], cos, sin).astype(BF)
        q_ref[part, hd:] = rotate(tq[:, hd:], cos, sin).astype(BF)
        k_ref[part, :] = rotate(dot_nn(n, wk_ref[...]) + bk_ref[...], cos, sin).astype(BF)
        v_ref[part, :] = (dot_nn(n, wv_ref[...]) + bv_ref[...]).astype(BF)

    factor = scale * LOG2E
    sink0 = sink_ref[layer, 2 * head] * LOG2E
    sink1 = sink_ref[layer, 2 * head + 1] * LOG2E
    for r, size, k0, k1, masked in spans(window_on, rows):
        part = slice(r, r + size)
        q2 = jnp.concatenate([q_ref[part, :hd], q_ref[part, hd:]], axis=0)
        mask = window_mask(masked, 2 * size) if window_on else causal_mask(masked, 2 * size)
        s = masked_logits(dot_nt(k_ref[k0:k1, :], q2) * factor, mask, masked)
        sink = jnp.where(lax.broadcasted_iota(jnp.int32, (1, 2 * size), 1) < size, sink0, sink1)
        peak = jnp.maximum(jnp.max(s, axis=0, keepdims=True), sink)
        e = jnp.exp2(s - peak)
        denom = jnp.sum(e, axis=0, keepdims=True) + jnp.exp2(sink - peak)
        p = (e * (1.0 / denom)).astype(BF)
        o = dot_tn(p, v_ref[k0:k1, :]).astype(BF)
        o_ref[part, :hd] = o[:size]
        o_ref[part, hd:] = o[size:]
        lse = peak + jnp.log(denom) * LOG2E
        lse_ref[0:1, part] = lse[:, :size]
        lse_ref[1:2, part] = lse[:, size:]


def forward_attention(layer, window_on, x, gain, w_qkv, b_qkv, cos, sin, sinks, heads, kv):
    rows, d = x.shape
    hd = w_qkv.shape[2] // (heads + 2 * kv)
    half = hd // 2
    once = pl.Buffered(1)
    whole = lambda h: (0, 0)
    in_specs = [
        pl.BlockSpec((rows, d), whole, pipeline_mode=once),
        pl.BlockSpec((None, 1, d), lambda h: (layer, 0, 0)),
        pl.BlockSpec((None, d, 2 * hd), lambda h: (layer, 0, h)),
        pl.BlockSpec((None, d, hd), lambda h: (layer, 0, heads + h)),
        pl.BlockSpec((None, d, hd), lambda h: (layer, 0, heads + kv + h)),
        pl.BlockSpec((None, 1, 2 * hd), lambda h: (layer, 0, h)),
        pl.BlockSpec((None, 1, hd), lambda h: (layer, 0, heads + h)),
        pl.BlockSpec((None, 1, hd), lambda h: (layer, 0, heads + kv + h)),
        pl.BlockSpec((rows, half), whole, pipeline_mode=once),
        pl.BlockSpec((rows, half), whole, pipeline_mode=once),
        pl.BlockSpec(memory_space=pltpu.SMEM),
    ]
    out_specs = [
        pl.BlockSpec((rows, 2 * hd), lambda h: (0, h)),
        pl.BlockSpec((rows, hd), lambda h: (0, h)),
        pl.BlockSpec((rows, hd), lambda h: (0, h)),
        pl.BlockSpec((rows, 2 * hd), lambda h: (0, h)),
        pl.BlockSpec((None, 2, rows), lambda h: (h, 0, 0)),
    ]
    out_shape = [
        jax.ShapeDtypeStruct((rows, heads * hd), BF),
        jax.ShapeDtypeStruct((rows, kv * hd), BF),
        jax.ShapeDtypeStruct((rows, kv * hd), BF),
        jax.ShapeDtypeStruct((rows, heads * hd), BF),
        jax.ShapeDtypeStruct((kv, 2, rows), F32),
    ]
    return pl.pallas_call(
        functools.partial(forward_kernel, layer, window_on, hd ** -0.5),
        grid=(kv,), in_specs=in_specs, out_specs=out_specs, out_shape=out_shape,
        scratch_shapes=[pltpu.VMEM((rows, d), BF)],
        compiler_params=pltpu.CompilerParams(dimension_semantics=("arbitrary",), vmem_limit_bytes=VMEM_LIMIT),
        cost_estimate=pl.CostEstimate(flops=2 * rows * d * w_qkv.shape[2] + 8 * rows * rows * heads * hd // 4, bytes_accessed=2 * d * w_qkv.shape[2], transcendentals=0),
    )(x, gain, w_qkv, w_qkv, w_qkv, b_qkv, b_qkv, b_qkv, cos, sin, sinks)


def backward_kernel(layer, window_on, scale, dy_ref, wo_ref, q_ref, k_ref, v_ref, lse_ref, cos_ref, sin_ref, sink_ref, dp_ref, db_ref, ds_ref, do_ref, dk_ref, dv_ref):
    head = pl.program_id(0)
    rows = dy_ref.shape[0]
    hd = k_ref.shape[1]
    chunk = rows // db_ref.shape[0]
    step = min(512, rows)
    for r in range(0, rows, step):
        do_ref[r:r + step, :] = dot_nt(dy_ref[r:r + step, :], wo_ref[...]).astype(BF)

    factor = scale * LOG2E
    sink0 = sink_ref[layer, 2 * head] * LOG2E
    sink1 = sink_ref[layer, 2 * head + 1] * LOG2E

    def finish(block, part, col, turn):
        f = block.astype(BF).astype(F32)
        if turn:
            f = rotate(f, cos_ref[part, :], -sin_ref[part, :])
        dp_ref[part, col:col + hd] = f.astype(BF)
        for i in range(0, f.shape[0], chunk):
            c = (part.start + i) // chunk
            db_ref[c:c + 1, col:col + hd] = jnp.sum(f[i:i + chunk], axis=0, keepdims=True)

    for r, size, k0, k1, masked in spans(window_on, rows):
        part = slice(r, r + size)
        q2 = jnp.concatenate([q_ref[part, :hd], q_ref[part, hd:]], axis=0)
        do2 = jnp.concatenate([do_ref[part, :hd], do_ref[part, hd:]], axis=0)
        lse = jnp.concatenate([lse_ref[0:1, part], lse_ref[1:2, part]], axis=1)
        keys, values = k_ref[k0:k1, :], v_ref[k0:k1, :]
        mask = window_mask(masked, 2 * size) if window_on else causal_mask(masked, 2 * size)
        s = masked_logits(dot_nt(keys, q2) * factor, mask, masked)
        p = jnp.exp2(s - lse)
        g = dot_nt(values, do2).astype(BF).astype(F32)
        delta = jnp.sum(p * g, axis=0, keepdims=True)
        ds = (p * (g - delta)).astype(BF)
        sink = jnp.where(lax.broadcasted_iota(jnp.int32, (1, 2 * size), 1) < size, sink0, sink1)
        sd = jnp.exp2(sink - lse) * delta
        ds_ref[0:1, part] = sd[:, :size]
        ds_ref[1:2, part] = sd[:, size:]
        dv = dot_nn(p.astype(BF), do2)
        dk = dot_nn(ds, q2)
        fresh = r + size == rows
        if fresh:
            dv_ref[k0:k1, :] = dv
            dk_ref[k0:k1, :] = dk
        elif window_on:
            own = k1 - size
            dv_ref[own:k1, :] += dv[own - k0:]
            dk_ref[own:k1, :] += dk[own - k0:]
            if own > k0:
                dv_ref[k0:own, :] = dv[:own - k0]
                dk_ref[k0:own, :] = dk[:own - k0]
        else:
            dv_ref[k0:k1, :] += dv
            dk_ref[k0:k1, :] += dk
        dq = dot_tn(ds, keys) * scale
        finish(dq[:size], part, 0, True)
        finish(dq[size:], part, hd, True)
        finish(dk_ref[part, :] * scale, part, 2 * hd, True)
        finish(dv_ref[part, :], part, 3 * hd, False)


def backward_attention(layer, window_on, dy, w_out, q, k, v, lse, cos, sin, sinks, chunks):
    rows, d = dy.shape
    kv = lse.shape[0]
    hd = k.shape[1] // kv
    half = hd // 2
    once = pl.Buffered(1)
    whole = lambda h: (0, 0)
    in_specs = [
        pl.BlockSpec((rows, d), whole, pipeline_mode=once),
        pl.BlockSpec((None, 2 * hd, d), lambda h: (layer, h, 0)),
        pl.BlockSpec((rows, 2 * hd), lambda h: (0, h)),
        pl.BlockSpec((rows, hd), lambda h: (0, h)),
        pl.BlockSpec((rows, hd), lambda h: (0, h)),
        pl.BlockSpec((None, 2, rows), lambda h: (h, 0, 0)),
        pl.BlockSpec((rows, half), whole, pipeline_mode=once),
        pl.BlockSpec((rows, half), whole, pipeline_mode=once),
        pl.BlockSpec(memory_space=pltpu.SMEM),
    ]
    out_specs = [
        pl.BlockSpec((None, rows, 4 * hd), lambda h: (h, 0, 0)),
        pl.BlockSpec((chunks, 4 * hd), lambda h: (0, h)),
        pl.BlockSpec((None, 2, rows), lambda h: (h, 0, 0)),
    ]
    out_shape = [
        jax.ShapeDtypeStruct((kv, rows, 4 * hd), BF),
        jax.ShapeDtypeStruct((chunks, kv * 4 * hd), F32),
        jax.ShapeDtypeStruct((kv, 2, rows), F32),
    ]
    return pl.pallas_call(
        functools.partial(backward_kernel, layer, window_on, hd ** -0.5),
        grid=(kv,), in_specs=in_specs, out_specs=out_specs, out_shape=out_shape,
        scratch_shapes=[pltpu.VMEM((rows, 2 * hd), BF), pltpu.VMEM((rows, hd), F32), pltpu.VMEM((rows, hd), F32)],
        compiler_params=pltpu.CompilerParams(dimension_semantics=("arbitrary",), vmem_limit_bytes=VMEM_LIMIT),
        cost_estimate=pl.CostEstimate(flops=2 * rows * d * 2 * kv * hd + 20 * rows * rows * 2 * kv * hd // 4, bytes_accessed=2 * d * 2 * kv * hd, transcendentals=0),
    )(dy, w_out, q, k, v, lse, cos, sin, sinks)


def input_kernel(chunk, dp_ref, wq_ref, wk_ref, wv_ref, x_ref, gain_ref, res_ref, out_ref, dg_ref, db_ref, acc_ref):
    step = pl.program_id(1)
    rows, d = acc_ref.shape
    tile = 768
    dp = dp_ref[...]

    def product(n):
        part = slice(n, n + tile)
        return dot_nt(dp, jnp.concatenate([wq_ref[part, :], wk_ref[part, :], wv_ref[part, :]], axis=1))

    @pl.when(step == 0)
    def _():
        for n in range(0, d, tile):
            acc_ref[:, n:n + tile] = product(n)

    @pl.when(step > 0)
    def _():
        for n in range(0, d, tile):
            acc_ref[:, n:n + tile] += product(n)

    @pl.when(step == pl.num_programs(1) - 1)
    def _():
        sub = 32
        gain = gain_ref[...]

        def finish(i, c):
            def piece(j, carry):
                dg, db = carry
                part = pl.ds(pl.multiple_of(i * chunk + j * sub, sub), sub)
                dn = acc_ref[part, :].astype(BF).astype(F32)
                f = x_ref[part, :].astype(F32)
                inv = lax.rsqrt(jnp.mean(f * f, axis=1, keepdims=True) + EPSILON)
                unit = dn * gain
                dot = jnp.mean(unit * f, axis=1, keepdims=True)
                dh = inv * unit - f * (inv * inv * inv * dot)
                out = (res_ref[part, :].astype(F32) + dh).astype(BF)
                out_ref[part, :] = out
                dg = dg + jnp.sum(dn * f * inv, axis=0, keepdims=True)
                db = db + jnp.sum(out.astype(F32), axis=0, keepdims=True)
                return dg, db

            zero = jnp.zeros((1, d), F32)
            dg, db = lax.fori_loop(0, chunk // sub, piece, (zero, zero))
            dg_ref[i] = dg
            db_ref[i] = db
            return c

        lax.fori_loop(0, rows // chunk, finish, 0)


def input_gradient(layer, dproj, w_qkv, x, gain, residual, heads, chunks):
    kv, rows, width = dproj.shape
    d = x.shape[1]
    hd = width // 4
    parts = 2
    m = rows // parts
    chunk = rows // chunks
    once = pl.Buffered(1)
    row = lambda i, h: (i, 0)
    in_specs = [
        pl.BlockSpec((None, m, width), lambda i, h: (h, i, 0)),
        pl.BlockSpec((None, d, 2 * hd), lambda i, h: (layer, 0, h)),
        pl.BlockSpec((None, d, hd), lambda i, h: (layer, 0, heads + h)),
        pl.BlockSpec((None, d, hd), lambda i, h: (layer, 0, heads + kv + h)),
        pl.BlockSpec((m, d), row),
        pl.BlockSpec((None, 1, d), lambda i, h: (layer, 0, 0)),
        pl.BlockSpec((m, d), row),
    ]
    out_specs = [
        pl.BlockSpec((m, d), row),
        pl.BlockSpec((m // chunk, 1, d), lambda i, h: (i, 0, 0)),
        pl.BlockSpec((m // chunk, 1, d), lambda i, h: (i, 0, 0)),
    ]
    out_shape = [
        jax.ShapeDtypeStruct((rows, d), BF),
        jax.ShapeDtypeStruct((chunks, 1, d), F32),
        jax.ShapeDtypeStruct((chunks, 1, d), F32),
    ]
    return pl.pallas_call(
        functools.partial(input_kernel, chunk),
        grid=(parts, kv), in_specs=in_specs, out_specs=out_specs, out_shape=out_shape,
        scratch_shapes=[pltpu.VMEM((m, d), F32)],
        compiler_params=pltpu.CompilerParams(dimension_semantics=("arbitrary", "arbitrary"), vmem_limit_bytes=VMEM_LIMIT),
        cost_estimate=pl.CostEstimate(flops=2 * rows * d * w_qkv.shape[2], bytes_accessed=4 * d * w_qkv.shape[2], transcendentals=0),
    )(dproj, w_qkv, w_qkv, w_qkv, x, gain, residual)


def solution(mesh):
    chunks = mesh.shape['cp']
    row_spec = P('dp', 'cp')
    device_spec = P(('dp', 'cp'))
    whole_spec = P()

    def step(hidden, grad_out, norm_gain, w_qkv, b_qkv, w_out, b_out, attn_sinks):
        batch, seq_dev, d = hidden.shape
        heads = attn_sinks.shape[1]
        hd = w_out.shape[1] // heads
        kv = (w_qkv.shape[2] // hd - heads) // 2
        rows = chunks * seq_dev
        cos, sin = rope_tables(jnp.arange(rows), hd)
        gain = norm_gain[:, None, :]
        bias = b_qkv[:, None, :]

        def exchange(block):
            return lax.all_to_all(block, 'cp', 0, 0, tiled=True)

        def total(parts):
            return jnp.sum(exchange(jnp.concatenate(parts, axis=1)), axis=0)

        x = exchange(hidden).reshape(rows, d)
        dy = exchange(grad_out).reshape(rows, d)

        def dense(layer, o, h):
            t = jnp.dot(o, w_out[layer], preferred_element_type=F32) + b_out[layer]
            return (h.astype(F32) + t).astype(BF)

        q1, k1, v1, o1, lse1 = forward_attention(0, True, x, gain, w_qkv, bias, cos, sin, attn_sinks, heads, kv)
        mid = dense(0, o1, x)
        q2, k2, v2, o2, lse2 = forward_attention(1, False, mid, gain, w_qkv, bias, cos, sin, attn_sinks, heads, kv)
        out_rows, dy = lax.optimization_barrier((dense(1, o2, mid), dy))
        output = exchange(out_rows.reshape(batch, seq_dev, d))

        def sink_rows(s):
            return -jnp.sum(s.reshape(heads, chunks, seq_dev), axis=2).T

        dproj2, dbias2, dsink2 = backward_attention(1, False, dy, w_out, q2, k2, v2, lse2, cos, sin, attn_sinks, chunks)
        d_mid, dgain2, dbout1 = input_gradient(1, dproj2, w_qkv, mid, gain, dy, heads, chunks)
        d_mid, output = lax.optimization_barrier((d_mid, output))
        dproj1, dbias1, dsink1 = backward_attention(0, True, d_mid, w_out, q1, k1, v1, lse1, cos, sin, attn_sinks, chunks)
        early = total([dbias2, dgain2[:, 0], dbout1[:, 0], sink_rows(dsink2)])
        dproj1, early = lax.optimization_barrier((dproj1, early))
        d_x, dgain1, _ = input_gradient(0, dproj1, w_qkv, x, gain, d_mid, heads, chunks)
        d_hidden = exchange(d_x.reshape(batch, seq_dev, d))

        wide = kv * 4 * hd
        late = total([dbias1, dgain1[:, 0], sink_rows(dsink1)])

        def split_bias(b):
            b = b.reshape(kv, 4 * hd)
            return jnp.concatenate([b[:, :2 * hd].reshape(-1), b[:, 2 * hd:3 * hd].reshape(-1), b[:, 3 * hd:].reshape(-1)])

        d_gain = jnp.stack([late[wide:wide + d], early[wide:wide + d]])[None]
        d_bias_qkv = jnp.stack([split_bias(late[:wide]), split_bias(early[:wide])])[None]
        d_bias_out = jnp.stack([early[wide + d:wide + 2 * d], jnp.sum(grad_out.astype(F32), axis=(0, 1))])[None]
        d_sinks = jnp.stack([late[wide + d:], early[wide + 2 * d:]])[None]
        return output, d_hidden, d_gain, d_bias_qkv, d_bias_out, d_sinks

    return jax.shard_map(step, mesh=mesh, in_specs=(row_spec, row_spec, whole_spec, whole_spec, whole_spec, whole_spec, whole_spec, whole_spec), out_specs=(row_spec, row_spec, device_spec, device_spec, device_spec, device_spec), check_vma=False)
```
